16 devices in a mesh: col: 4 (over z, y), row: 4 (over x, core).
Axes of the slice: x: 2, y: 2, z: 2, core: 2. Of those that a mesh axis runs over, the one named last changes fastest.
Arguments:
- psi_init: float32 [3072, 2, 3072], P('row', None, 'col')
- left_env: float32 [3072, 8, 3072], P('row')
- mpo_tensor: float32 [8, 8, 2, 2], replicated
- right_env: float32 [3072, 8, 3072], P('col')
Outputs:
- output 1: float32 [4], replicated
- output 2: float32 [4], replicated
- output 3: float32 [3072, 2, 3072], P('row', None, 'col')
All inputs are finite; a program needn't handle non-finite values.
Results may differ from the reference program's by a relative error of at most 0.001.
Values sent between devices are 32-bit elements.
A program may use at most 1 GiB of HBM per device.

```python
import jax
import jax.numpy as jnp
from jax import lax

BOND_DIM = 3072
PHYS_DIM = 2
MPO_DIM = 8
LANCZOS_STEPS = 4
REF_BLOCK = min(BOND_DIM, 128)
EXACT_PREC = lax.Precision.HIGHEST


def make_env(key_dense, key_shift):
    dense_part = jax.random.normal(key_dense, (BOND_DIM, MPO_DIM, BOND_DIM), jnp.float32)
    dense_part = (dense_part + jnp.transpose(dense_part, (2, 1, 0))) * (0.5 / BOND_DIM) ** 0.5
    shifts = 1.0 + 0.5 * jax.random.normal(key_shift, (MPO_DIM,), jnp.float32)
    eye_mat = jnp.eye(BOND_DIM, dtype=jnp.float32)
    return dense_part + eye_mat[:, None, :] * shifts[None, :, None]


def setup_inputs(seed: int = 0) -> dict:
    key_list = jax.random.split(jax.random.key(seed), 6)
    psi_init = jax.random.normal(key_list[0], (BOND_DIM, PHYS_DIM, BOND_DIM), jnp.float32)
    left_env = make_env(key_list[1], key_list[2])
    mpo_raw = jax.random.normal(key_list[3], (MPO_DIM, MPO_DIM, PHYS_DIM, PHYS_DIM), jnp.float32)
    mpo_tensor = (mpo_raw + jnp.transpose(mpo_raw, (0, 1, 3, 2))) * (0.5 ** 0.5 / (MPO_DIM * PHYS_DIM ** 0.5))
    mpo_tensor = mpo_tensor + jnp.eye(PHYS_DIM, dtype=jnp.float32) / MPO_DIM ** 2
    right_env = make_env(key_list[4], key_list[5])
    return {"psi_init": psi_init, "left_env": left_env, "mpo_tensor": mpo_tensor, "right_env": right_env}


def apply_ham(vec_in, left_blocks, mpo_tensor, right_env):
    def one_block(left_blk):
        t_one = jnp.einsum("alc,asb->lcsb", left_blk, vec_in, precision=EXACT_PREC)
        t_two = jnp.einsum("lcsb,lrst->cbrt", t_one, mpo_tensor, precision=EXACT_PREC)
        return jnp.einsum("cbrt,brd->ctd", t_two, right_env, precision=EXACT_PREC)
    out_blocks = lax.map(one_block, left_blocks)
    return out_blocks.reshape(BOND_DIM, PHYS_DIM, BOND_DIM)


def reference(psi_init, left_env, mpo_tensor, right_env):
    block_count = BOND_DIM // REF_BLOCK
    left_blocks = jnp.transpose(left_env.reshape(BOND_DIM, MPO_DIM, block_count, REF_BLOCK), (2, 0, 1, 3))
    vec_init = psi_init / jnp.sqrt(jnp.sum(psi_init * psi_init))

    def lanczos_step(loop_state, step_input):
        vec_prev, vec_cur, beta_prev = loop_state
        work_vec = apply_ham(vec_cur, left_blocks, mpo_tensor, right_env)
        alpha_val = jnp.sum(vec_cur * work_vec)
        work_vec = work_vec - alpha_val * vec_cur - beta_prev * vec_prev
        beta_val = jnp.sqrt(jnp.sum(work_vec * work_vec))
        return (vec_cur, work_vec / beta_val, beta_val), (alpha_val, beta_val)

    state_init = (jnp.zeros_like(vec_init), vec_init, jnp.zeros((), vec_init.dtype))
    final_state, scalar_lists = lax.scan(lanczos_step, state_init, None, length=LANCZOS_STEPS)
    return scalar_lists[0], scalar_lists[1], final_state[1]
```

```python
import jax
import jax.numpy as jnp
from jax import lax
from jax.experimental import pallas as pl
from jax.experimental.layout import Layout, with_layout_constraint
from jax.experimental.pallas import tpu as pltpu
from jax.sharding import PartitionSpec as P


LANCZOS_STEPS = 4
EXACT_PREC = lax.Precision.HIGHEST
LANES = 128
SUBLANES = 8
MPO_ROWS = 16


def solution(mesh):
    row_count = mesh.shape["row"]
    col_count = mesh.shape["col"]
    axis_names = tuple(mesh.axis_names)
    dev_count = row_count * col_count

    def sum_kernel(part_ref, out_ref, slots, send_sem, recv_sem):
        row_me = lax.axis_index("row")
        col_me = lax.axis_index("col")
        me = col_me * row_count + row_me

        def coords(shift):
            peer = lax.rem(me + shift, dev_count)
            where = {"col": peer // row_count, "row": lax.rem(peer, row_count)}
            return tuple(where[name] for name in axis_names)

        barrier = pltpu.get_barrier_semaphore()
        for shift in range(1, dev_count):
            pl.semaphore_signal(barrier, inc=1, device_id=coords(shift), device_id_type=pl.DeviceIdType.MESH)
        pl.semaphore_wait(barrier, dev_count - 1)
        copies = []
        for shift in range(1, dev_count):
            copies.append(pltpu.make_async_remote_copy(
                src_ref=part_ref,
                dst_ref=slots.at[me],
                send_sem=send_sem.at[shift],
                recv_sem=recv_sem.at[shift],
                device_id=coords(shift),
                device_id_type=pl.DeviceIdType.MESH,
            ))
            copies[-1].start()
        slots[me] = part_ref[...]
        for copy in copies:
            copy.wait()
        total = slots[0]
        for dev in range(1, dev_count):
            total = total + slots[dev]
        out_ref[...] = total

    call_ids = iter(range(64))

    def global_sum(part):
        tile = jnp.full((SUBLANES, LANES), part, jnp.float32)
        total = pl.pallas_call(
            sum_kernel,
            out_shape=jax.ShapeDtypeStruct((SUBLANES, LANES), jnp.float32),
            in_specs=[pl.BlockSpec(memory_space=pltpu.VMEM)],
            out_specs=pl.BlockSpec(memory_space=pltpu.VMEM),
            scratch_shapes=[
                pltpu.VMEM((dev_count, SUBLANES, LANES), jnp.float32),
                pltpu.SemaphoreType.DMA((dev_count,)),
                pltpu.SemaphoreType.DMA((dev_count,)),
            ],
            compiler_params=pltpu.CompilerParams(collective_id=next(call_ids), has_side_effects=True),
            name="global_sum",
        )(tile)
        return total[0, 0]

    def mpo_kernel(mpo_ref, one_ref, two_ref):
        phys, bonds, rows = one_ref.shape[:3]
        for start in range(0, rows, SUBLANES):
            for t_idx in range(phys):
                planes = []
                for r_idx in range(bonds):
                    total = None
                    for s_idx in range(phys):
                        for l_idx in range(bonds):
                            weight = mpo_ref[((l_idx * bonds + r_idx) * phys + s_idx) * phys + t_idx]
                            term = weight * one_ref[s_idx, l_idx, start:start + SUBLANES]
                            total = term if total is None else total + term
                    planes.append(total)
                two_ref[start:start + SUBLANES, t_idx] = jnp.swapaxes(jnp.stack(planes, 0), 0, 1)

    def apply_mpo(t_one, mpo_tensor):
        phys, bonds, b_len, c_len = t_one.shape
        return pl.pallas_call(
            mpo_kernel,
            grid=(b_len // MPO_ROWS,),
            in_specs=[
                pl.BlockSpec(memory_space=pltpu.SMEM),
                pl.BlockSpec((phys, bonds, MPO_ROWS, c_len), lambda i: (0, 0, i, 0)),
            ],
            out_specs=pl.BlockSpec((MPO_ROWS, phys, bonds, c_len), lambda i: (i, 0, 0, 0)),
            out_shape=jax.ShapeDtypeStruct((b_len, phys, bonds, c_len), jnp.float32),
            cost_estimate=pl.CostEstimate(flops=2 * phys * bonds * t_one.size, bytes_accessed=8 * t_one.size, transcendentals=0),
            name="apply_mpo",
        )(mpo_tensor.reshape(-1), t_one)

    def shifted(blk, axis, count, shift):
        return lax.ppermute(blk, axis, [(i, (i + shift) % count) for i in range(count)])

    def local_steps(psi_blk, left_blk, mpo_tensor, right_blk):
        a_loc = psi_blk.shape[0]
        b_loc = psi_blk.shape[2]
        row_me = lax.axis_index("row")
        col_me = lax.axis_index("col")
        left_parts = {}
        for shift in range(row_count):
            src = lax.rem(row_me + row_count - shift, row_count)
            left_parts[shift] = lax.dynamic_slice_in_dim(left_blk, src * a_loc, a_loc, axis=2)
        right_parts = {}
        for shift in range(col_count):
            dst = lax.rem(col_me + shift, col_count)
            right_parts[shift] = with_layout_constraint(lax.dynamic_slice_in_dim(right_blk, dst * b_loc, b_loc, axis=2), Layout(major_to_minor=(0, 1, 2)))

        def apply_ham(vec_blk, left_parts):
            order = [0, 1] + list(range(row_count - 1, 1, -1))
            vecs = {0: vec_blk}
            for shift in order[1:]:
                vecs[shift] = shifted(vec_blk, "row", row_count, shift)
            t_one = None
            for shift in order:
                part = jnp.einsum("cla,asb->slbc", left_parts[shift], vecs[shift], precision=EXACT_PREC, preferred_element_type=jnp.float32)
                t_one = part if t_one is None else t_one + part
            t_two = apply_mpo(t_one, mpo_tensor)
            landed = []
            for shift in range(1, col_count):
                y_part = jnp.einsum("btrc,brd->tdc", t_two, right_parts[shift], precision=EXACT_PREC, preferred_element_type=jnp.float32)
                landed.append(shifted(y_part, "col", col_count, shift))
            total = jnp.einsum("btrc,brd->tdc", t_two, right_parts[0], precision=EXACT_PREC, preferred_element_type=jnp.float32)
            total = lax.optimization_barrier(total)
            for part in landed:
                total = total + part
            return jnp.transpose(total, (2, 0, 1))

        vec_cur = psi_blk / jnp.sqrt(global_sum(jnp.sum(psi_blk * psi_blk)))
        vec_prev = jnp.zeros_like(vec_cur)
        beta_prev = jnp.zeros((), jnp.float32)
        alpha_list = []
        beta_list = []
        for _ in range(LANCZOS_STEPS):
            vec_cur, left_parts = lax.optimization_barrier((vec_cur, left_parts))
            work_vec = apply_ham(vec_cur, left_parts)
            alpha_val = global_sum(jnp.sum(vec_cur * work_vec))
            work_vec = work_vec - alpha_val * vec_cur - beta_prev * vec_prev
            beta_val = jnp.sqrt(global_sum(jnp.sum(work_vec * work_vec)))
            vec_prev = vec_cur
            vec_cur = work_vec / beta_val
            beta_prev = beta_val
            alpha_list.append(alpha_val)
            beta_list.append(beta_val)
        return jnp.stack(alpha_list), jnp.stack(beta_list), vec_cur

    return jax.shard_map(local_steps, mesh=mesh, in_specs=(P("row", None, "col"), P("row", None, None), P(), P("col", None, None)), out_specs=(P(), P(), P("row", None, "col")), check_vma=False)
```
